32 devices in a mesh: scan: 2 (over y), chan: 4 (over z), tm: 2 (over x), pol: 2 (over core).
Axes of the slice: x: 2, y: 2, z: 4, core: 2. Of those that a mesh axis runs over, the one named last changes fastest.
Arguments:
- samples: int32 [2, 8, 4, 2, 16, 32768], P('pol', ('scan', 'tm'), None, None, None, 'chan'), parts along dimension 1, may hold values from 0 to 3
- pcal_phase: float32 [2, 16, 128], P('pol'), may hold values from -3.140625 to 3.140625
- tone_index: int32 [32768], P('chan'), may hold values from 0 to 127
- baseline_pairs: int32 [120, 2], replicated, may hold values from 0 to 15, as said below
Outputs:
- fringe_power: float32 [2, 8, 120, 8192], P('pol', ('scan', 'chan'), 'tm'), parts along dimension 1
The draws below stay inside these ranges and needn't reach their ends.
There are 2 independent parts, one for each index of `scan`. The reference program is written for one: setup_inputs(seed, part) draws one part's arguments, and reference() takes and returns one part's arrays. A program takes and returns all parts, laid end to end along the dimension named above; an argument that names none is the same for every part. Nothing has to cross between parts.
Inputs may be any that keep to these rules, and one draw needn't show every extreme that they name: `baseline_pairs`: each row holds two different stations; every unordered pair of the 16 stations stands in exactly one row, in either order.
All inputs are finite; a program needn't handle non-finite values.
Results may differ from the reference program's by a relative error of at most 0.0029.
Values may be sent and summed in bfloat16 or wider, within the bound.
A program may use at most 256 MiB of HBM per device.

```python
import jax
import jax.numpy as jnp
import numpy as np
from jax import lax

S = 16
NC = 32768
NTONE = 128
M = 4
NPOL = 2
NT = 4
ND = 8192


def draw_baseline_pairs(key, part):
    pair_table = np.array([(low_station, high_station) for low_station in range(S) for high_station in range(low_station + 1, S)], dtype=np.int32)
    pair_order = jax.random.permutation(key, pair_table.shape[0])
    picked_rows = jnp.asarray(pair_table)[pair_order]
    flipped = jax.random.randint(jax.random.fold_in(key, 7), (pair_table.shape[0],), 0, 2)
    first_station = jnp.where(flipped == 1, picked_rows[:, 1], picked_rows[:, 0])
    second_station = jnp.where(flipped == 1, picked_rows[:, 0], picked_rows[:, 1])
    return jnp.stack([first_station, second_station], axis=1).astype(jnp.int32)


def with_ends(result, stream_key, smallest, high):
    longest = result.shape.index(max(result.shape))
    spots = []
    for shift in (0, 1):
        where = [jax.random.randint(jax.random.fold_in(stream_key, axis), (), 0, length) for axis, length in enumerate(result.shape)]
        where[longest] = (where[longest] + shift) % result.shape[longest]
        spots.append(tuple(where))
    return result.at[spots[0]].set(smallest).at[spots[1]].set(high)


def setup_inputs(seed: int = 0, part: int = 0) -> dict:
    seeds = jax.random.split(jax.random.key(seed), 5)
    part_splits = jax.random.split(jax.random.fold_in(seeds[4], part), 5)
    return {
        "samples": with_ends(jax.random.randint(part_splits[0], (NPOL, NT, M, 2, S, NC), 0, 4), jax.random.fold_in(part_splits[0], 1), 0, 3).astype(jnp.int32),
        "pcal_phase": jnp.clip(jax.random.uniform(seeds[1], (NPOL, S, NTONE), jnp.float32, -3.140625, 3.140625), -3.140625, 3.140625),
        "tone_index": with_ends(jax.random.randint(seeds[2], (NC,), 0, NTONE), jax.random.fold_in(seeds[2], 1), 0, NTONE - 1).astype(jnp.int32),
        "baseline_pairs": draw_baseline_pairs(jax.random.fold_in(seeds[4], 71), part),
    }


def calibrated_period(block, first_index, second_index, cos_diff, sin_diff):
    levels = (2 * block - 3).astype(jnp.float32)
    first_volts = levels[:, :, first_index, :]
    second_volts = levels[:, :, second_index, :]
    raw_real = jnp.sum(first_volts[:, 0] * second_volts[:, 0] + first_volts[:, 1] * second_volts[:, 1], axis=0)
    raw_imag = jnp.sum(first_volts[:, 1] * second_volts[:, 0] - first_volts[:, 0] * second_volts[:, 1], axis=0)
    vis_real = raw_real * cos_diff + raw_imag * sin_diff
    vis_imag = raw_imag * cos_diff - raw_real * sin_diff
    return jnp.stack([vis_real, vis_imag], axis=1).astype(jnp.bfloat16)


def one_polarization(samples_pol, phase_pol, tone_index, baseline_pairs):
    first_index = baseline_pairs[:, 0]
    second_index = baseline_pairs[:, 1]
    cos_table = jnp.cos(phase_pol)[:, tone_index]
    sin_table = jnp.sin(phase_pol)[:, tone_index]
    cos_first = cos_table[first_index]
    sin_first = sin_table[first_index]
    cos_second = cos_table[second_index]
    sin_second = sin_table[second_index]
    cos_diff = cos_first * cos_second + sin_first * sin_second
    sin_diff = sin_first * cos_second - cos_first * sin_second

    def per_period(block):
        return calibrated_period(block, first_index, second_index, cos_diff, sin_diff)

    visibility = lax.map(per_period, samples_pol)
    values = visibility.astype(jnp.float32)
    spectra = jnp.fft.fft(lax.complex(values[:, :, 0], values[:, :, 1]), axis=0)
    lag_index = (jnp.arange(ND, dtype=jnp.int32) - ND // 2) % NC
    scale = 1.0 / (100.0 * M * NT * NC)

    def per_rate(rate_row):
        delays = jnp.fft.fft(rate_row, axis=-1)[:, lag_index]
        return (jnp.real(delays) * jnp.real(delays) + jnp.imag(delays) * jnp.imag(delays)) * scale

    return lax.map(per_rate, spectra)


def reference(samples, pcal_phase, tone_index, baseline_pairs):
    outputs = [one_polarization(samples[pol_index], pcal_phase[pol_index], tone_index, baseline_pairs) for pol_index in range(NPOL)]
    return jnp.stack(outputs, axis=0).astype(jnp.float32)
```

```python
import functools
import math

import jax
import jax.numpy as jnp
from jax import lax
from jax.experimental import pallas as pl
from jax.experimental.pallas import tpu as pltpu
from jax.sharding import PartitionSpec as P


S = 16
C1 = 128
WD1 = 32
NTONE = 128
CHUNKS = 5

highest = lax.Precision.HIGHEST
two_pi = 2.0 * math.pi
f32, bf16 = jnp.float32, jnp.bfloat16


def phase_table(left, right, modulus):
    product = left[:, None] * right[None, :] % modulus
    angles = two_pi * product.astype(f32) / modulus
    return (jnp.cos(angles), jnp.sin(angles))


def split_hi_lo(value):
    high = lax.reduce_precision(value, 8, 7)
    return high.astype(bf16), (value - high).astype(bf16)


def correlate_kernel(pairs, x_ref, cos_ref, sin_ref, out_ref):
    periods, samples = x_ref.shape[0], x_ref.shape[1]
    depth = x_ref.shape[4]

    @pl.loop(0, out_ref.shape[1])
    def _(row):
        a = pairs[row, 0]
        e = pairs[row, 1]
        ca, sa = cos_ref[a], sin_ref[a]
        ce, se = cos_ref[e], sin_ref[e]
        cos_diff = ca * ce + sa * se
        sin_diff = sa * ce - ca * se
        for period in range(periods):
            real = imag = None
            for m in range(samples):
                ar, ai = x_ref[period, m, 0, a], x_ref[period, m, 1, a]
                er, ei = x_ref[period, m, 0, e], x_ref[period, m, 1, e]
                step_real = ar * er + ai * ei
                step_imag = ai * er - ar * ei
                real = step_real if real is None else real + step_real
                imag = step_imag if imag is None else imag + step_imag
            real, imag = real.astype(f32), imag.astype(f32)
            out_ref[period, row, :depth] = (real * cos_diff + imag * sin_diff).astype(bf16)
            out_ref[period, row, depth:] = (imag * cos_diff - real * sin_diff).astype(bf16)


def correlate(pairs, x, cosine, sine):
    periods, samples, _, _, depth, lanes = x.shape
    count = pairs.shape[0]
    return pl.pallas_call(
        correlate_kernel,
        out_shape=jax.ShapeDtypeStruct((periods, count, 2 * depth, lanes), bf16),
        in_specs=[
            pl.BlockSpec(memory_space=pltpu.SMEM),
            pl.BlockSpec(memory_space=pltpu.VMEM),
            pl.BlockSpec(memory_space=pltpu.VMEM),
            pl.BlockSpec(memory_space=pltpu.VMEM),
        ],
        out_specs=pl.BlockSpec(memory_space=pltpu.VMEM),
        compiler_params=pltpu.CompilerParams(vmem_limit_bytes=32 << 20),
        cost_estimate=pl.CostEstimate(
            flops=count * periods * samples * 8 * depth * lanes,
            bytes_accessed=x.size * 2 + count * periods * depth * lanes * 4,
            transcendentals=0,
        ),
        name="correlate",
    )(pairs, x, cosine, sine)


def add_scaled(total, value, factor):
    if abs(factor) < 1e-9:
        return total
    if abs(factor - 1.0) < 1e-9:
        return value if total is None else total + value
    if abs(factor + 1.0) < 1e-9:
        return -value if total is None else total - value
    return value * factor if total is None else total + value * factor


def delay_kernel(n_slots, rates, group, z_ref, *refs):
    slots = refs[:n_slots]
    first_ref, cos_ref, sin_ref, last_ref, keep_ref, send_ref, spectra = refs[n_slots:]
    per_slot = slots[0].shape[0]
    depth = slots[0].shape[2] // 2
    outer = cos_ref.shape[0]
    wide = last_ref.shape[0] // 2
    z = z_ref[0]
    for b in range(group):
        parts = []
        for slot in range(n_slots):
            for period in range(per_slot):
                value = slots[slot][period, b].astype(f32)
                parts.append(((period - per_slot * slot) % rates, value[:depth], value[depth:]))
        for rate in range(rates):
            real = imag = None
            for when, vr, vi in parts:
                angle = two_pi * (rate * when % rates) / rates
                c, s = math.cos(angle), math.sin(angle)
                real = add_scaled(real, vr, c)
                real = add_scaled(real, vi, s)
                imag = add_scaled(imag, vi, c)
                imag = add_scaled(imag, vr, -s)
            value = jnp.concatenate([real, imag], axis=0)
            high = value.astype(bf16)
            low = (value - high.astype(f32)).astype(bf16)
            spectra[rate, :, b * C1 : (b + 1) * C1] = jnp.concatenate([high, low, high], axis=0)
    for q in range(rates):
        section = jnp.dot(first_ref[...], spectra[z ^ q], preferred_element_type=f32)
        for b in range(group):
            yr = section[:outer, b * C1 : (b + 1) * C1]
            yi = section[outer:, b * C1 : (b + 1) * C1]
            tr = yr * cos_ref[...] + yi * sin_ref[...]
            ti = yi * cos_ref[...] - yr * sin_ref[...]
            twisted = jnp.concatenate([tr.astype(bf16), ti.astype(bf16)], axis=1)
            last = lax.dot_general(
                last_ref[...], twisted, (((1,), (1,)), ((), ())), preferred_element_type=f32
            )
            partial = last[:wide] + last[wide:]
            if q % 2 == 0:
                keep_ref[q // 2, b] = partial
            else:
                send_ref[q // 2, b] = partial.astype(bf16)


def delay_partial(z, slots, first, twist_cos, twist_sin, last, rates):
    n_slots = len(slots)
    periods, count, tall, lanes = slots[0].shape
    group = 2 if count % 2 == 0 else 1
    outer = twist_cos.shape[0]
    wide = last.shape[0] // 2
    whole = lambda shape: pl.BlockSpec(shape, lambda i: (0,) * len(shape))
    half = pl.BlockSpec((rates // 2, group, wide, outer), lambda i: (0, i, 0, 0))
    flops = count * rates * 2 * (first.size * lanes + last.size * outer)
    return pl.pallas_call(
        functools.partial(delay_kernel, n_slots, rates, group),
        grid=(count // group,),
        out_shape=(
            jax.ShapeDtypeStruct((rates // 2, count, wide, outer), f32),
            jax.ShapeDtypeStruct((rates // 2, count, wide, outer), bf16),
        ),
        in_specs=[pl.BlockSpec(memory_space=pltpu.SMEM)]
        + [pl.BlockSpec((periods, group, tall, lanes), lambda i: (0, i, 0, 0))] * n_slots
        + [whole(first.shape), whole(twist_cos.shape), whole(twist_sin.shape), whole(last.shape)],
        out_specs=(half, half),
        scratch_shapes=[pltpu.VMEM((rates, 3 * tall, group * lanes), bf16)],
        compiler_params=pltpu.CompilerParams(vmem_limit_bytes=32 << 20),
        cost_estimate=pl.CostEstimate(
            flops=4 * flops,
            bytes_accessed=count * (rates * wide * outer * 3 + n_slots * periods * tall * lanes * 2),
            transcendentals=0,
        ),
        name="delay",
    )(z, *slots, first, twist_cos, twist_sin, last)


def shards(samples, pcal_phase, tone_index, baseline_pairs):
    n_tm = lax.axis_size("tm")
    n_chan = lax.axis_size("chan")
    me = lax.axis_index("tm")
    z = lax.axis_index("chan").astype(jnp.int32)
    _, nt_dev, m, _, _, width = samples.shape
    rates = nt_dev * n_tm
    channels = width * n_chan
    outer = channels // C1
    depth = width // C1
    count = baseline_pairs.shape[0] // n_tm
    chunks = max(c for c in range(1, CHUNKS + 1) if count % c == 0)
    size = count // chunks

    x = (2 * samples[0] - 3).astype(bf16).reshape(nt_dev, m, 2, S, depth, C1)
    tone_slots = (tone_index[None, :] == jnp.arange(NTONE, dtype=jnp.int32)[:, None]).astype(f32)
    cosine = jnp.dot(jnp.cos(pcal_phase[0]), tone_slots, precision=highest).reshape(S, depth, C1)
    sine = jnp.dot(jnp.sin(pcal_phase[0]), tone_slots, precision=highest).reshape(S, depth, C1)

    outer_axis = jnp.arange(outer, dtype=jnp.int32)
    inner_axis = jnp.arange(C1, dtype=jnp.int32)
    kept_rows = jnp.concatenate(
        [jnp.arange(C1 - WD1 // 2, C1, dtype=jnp.int32), jnp.arange(WD1 // 2, dtype=jnp.int32)]
    )
    own_rows = z * depth + jnp.arange(depth, dtype=jnp.int32)
    fc, fs = phase_table(outer_axis, own_rows, outer)
    first = jnp.concatenate(
        [jnp.concatenate([fc, fs], axis=1), jnp.concatenate([-fs, fc], axis=1)], axis=0
    )
    first_hi, first_lo = split_hi_lo(first)
    first = jnp.concatenate([first_hi, first_hi, first_lo], axis=1)
    twist_cos, twist_sin = phase_table(outer_axis, inner_axis, channels)
    lc, ls = phase_table(kept_rows, inner_axis, C1)
    last = jnp.concatenate(
        [jnp.concatenate([lc, ls], axis=1), jnp.concatenate([-ls, lc], axis=1)], axis=0
    )
    last = jnp.concatenate(split_hi_lo(last), axis=0)
    scale = 1.0 / (100.0 * m * rates * channels)

    by_owner = jnp.roll(baseline_pairs.reshape(n_tm, count, 2), -me, axis=0)
    powers = []
    for chunk in range(chunks):
        pairs = by_owner[:, chunk * size : (chunk + 1) * size]
        slots = []
        for slot in range(n_tm):
            block = correlate(pairs[slot], x, cosine, sine)
            if slot:
                ring = [(i, (i + slot) % n_tm) for i in range(n_tm)]
                block = lax.ppermute(block, "tm", ring)
            slots.append(block)
        keep, send = delay_partial(
            z.reshape(1), slots, first, twist_cos, twist_sin, last, rates
        )
        step = 1
        while step < n_chan:
            swap = [(i, i ^ step) for i in range(n_chan)]
            keep = keep + lax.ppermute(send, "chan", swap).astype(f32)
            step *= 2
            if step < n_chan:
                send = keep[1::2].astype(bf16)
                keep = keep[0::2]
        half = keep.shape[2] // 2
        power = (keep[:, :, :half] ** 2 + keep[:, :, half:] ** 2) * scale
        powers.append(power.reshape(keep.shape[0], size, half * outer))
    return jnp.concatenate(powers, axis=1)[None]


def solution(mesh):
    placed = (
        P("pol", ("scan", "tm"), None, None, None, "chan"),
        P("pol", None, None),
        P("chan"),
        P(),
    )
    return jax.shard_map(
        shards,
        mesh=mesh,
        in_specs=placed,
        out_specs=P("pol", ("scan", "chan"), "tm", None),
        check_vma=False,
    )
```
